32 devices in a mesh: dp: 16 (over z, y, x), tensor: 2 (over core).
Axes of the slice: x: 2, y: 2, z: 4, core: 2. Of those that a mesh axis runs over, the one named last changes fastest.
Arguments:
- streams: bfloat16 [2048, 4, 8192], P('dp', None, 'tensor'), may hold values from -6 to 6
- layer_out: bfloat16 [2048, 8192], P('dp', 'tensor'), may hold values from -6 to 6
- cotangent: bfloat16 [2048, 4, 8192], P('dp', None, 'tensor'), may hold values from -6 to 6
- input_cot: bfloat16 [2048, 8192], P('dp', 'tensor'), may hold values from -6 to 6
- gain: float32 [8192], P('tensor'), may hold values from 0.5 to 1.5
- projection: float32 [6, 8192], P(None, 'tensor'), may hold values from -0.0625 to 0.0625
- static_mix: float32 [4, 6], replicated, may hold values from -3 to 3
- tanh_scale: float32 [3], replicated, may hold values from 0.5 to 2
Outputs:
- stream_grad: bfloat16 [2048, 4, 8192], P('dp', None, 'tensor')
- out_grad: bfloat16 [2048, 8192], P('dp', 'tensor')
- proj_grad: float32 [6, 8192], P(None, 'tensor')
- gain_grad: float32 [8192], P('tensor')
The draws below stay inside these ranges and needn't reach their ends.
All inputs are finite; a program needn't handle non-finite values.
Results may differ from the reference program's by a relative error of at most 0.0018.
Values sent between devices are 32-bit elements; how exact they have to be, the bound alone decides.
No kernel may reach another device: no remote copies, remote signals or barrier semaphores. Data moves between devices by JAX's collectives and lax.ppermute only.
A program may use at most 64 MiB of HBM per device.

```python
import math
import jax
import jax.numpy as jnp
from jax import lax

D = 8192
STREAMS = 4
TOKENS = 2048


def steps_of(own_key, extent, shards, least, largest):
    def one(position, blocks):
        draws = jax.random.uniform(jax.random.fold_in(jax.random.fold_in(own_key, 6), position), (blocks,), jnp.float32, least / len(shards), largest / len(shards))
        return jnp.repeat(jnp.exp(draws), extent[position] // blocks).reshape((-1,) + (1,) * (len(extent) - position - 1))

    factor_of = one(*shards[0])
    for cut in shards[1:]:
        factor_of = factor_of * one(*cut)
    return factor_of


def centred(key, extent, spread, most, cuts=(), held_as=jnp.bfloat16):
    drawn = jax.random.normal(key, extent, jnp.float32) * spread
    if len(cuts) > 0:
        drawn = steps_of(key, extent, cuts, -0.22, 0.18) * drawn
    return jnp.clip(drawn, min=-most, max=most).astype(held_as)


def setup_inputs(seed: int = 0) -> dict:
    arg_keys = jax.random.split(jax.random.key(seed), 9)
    return {
        "streams": centred(arg_keys[0], (TOKENS, STREAMS, D), 1.0, 6.0, ((0, 16), (2, 2))),
        "layer_out": centred(arg_keys[1], (TOKENS, D), 1.0, 6.0, ((0, 16), (1, 2))),
        "cotangent": centred(arg_keys[2], (TOKENS, STREAMS, D), 1.0, 6.0, ((0, 16), (2, 2))),
        "input_cot": centred(arg_keys[3], (TOKENS, D), 1.0, 6.0, ((0, 16), (1, 2))),
        "gain": jnp.clip(1.0 + 0.1 * jax.random.normal(arg_keys[4], (D,), jnp.float32), 0.5, 1.5),
        "projection": centred(arg_keys[5], (6, D), D ** -0.5, 0.0625, ((1, 2),), jnp.float32),
        "static_mix": centred(arg_keys[6], (STREAMS, 6), 0.5, 3.0, (), jnp.float32),
        "tanh_scale": jnp.clip(jnp.exp(jax.random.uniform(arg_keys[7], (3,), jnp.float32, math.log(0.5), math.log(2.0))), 0.5, 2.0),
    }


def reference(streams, layer_out, cotangent, input_cot, gain, projection, static_mix, tanh_scale):
    hidden = streams.astype(jnp.float32)
    grads = cotangent.astype(jnp.float32)
    output = layer_out.astype(jnp.float32)
    back_in = input_cot.astype(jnp.float32)
    wproj = gain[None, :] * projection
    square = jnp.einsum('tjd,tjd->tj', hidden, hidden, precision=lax.Precision.HIGHEST)
    lin = jnp.einsum('tjd,cd->tjc', hidden, wproj, precision=lax.Precision.HIGHEST)
    dbeta = jnp.einsum('td,tkd->tk', output, grads, precision=lax.Precision.HIGHEST)
    dalpha = jnp.einsum('tjd,td->tj', hidden, back_in, precision=lax.Precision.HIGHEST)
    dmixer = jnp.einsum('tjd,tkd->tjk', hidden, grads, precision=lax.Precision.HIGHEST)
    inv_rms = lax.rsqrt(square / D + 1e-06)
    bent = jnp.tanh(inv_rms[..., None] * lin)
    scales = jnp.concatenate([tanh_scale[0:2], jnp.repeat(tanh_scale[2:3], 4)])
    coef = static_mix[None] + scales * bent
    dcoef = jnp.concatenate([dbeta[..., None], dalpha[..., None], dmixer], axis=-1)
    dpre = dcoef * scales * (1.0 - bent * bent)
    dlin = dpre * inv_rms[..., None]
    dsquare = -0.5 * inv_rms ** 3 / D * lax.optimization_barrier(jnp.sum(dpre * lin, axis=-1))
    out_grad = jnp.einsum('tk,tkd->td', coef[:, :, 0], grads, precision=lax.Precision.HIGHEST).astype(jnp.bfloat16)
    total = jnp.einsum('tjk,tkd->tjd', coef[:, :, 2:], grads, precision=lax.Precision.HIGHEST)
    total = total + coef[:, :, 1][..., None] * back_in[:, None, :]
    total = total + jnp.einsum('tjc,cd->tjd', dlin, wproj, precision=lax.Precision.HIGHEST)
    total = total + 2.0 * dsquare[..., None] * hidden
    stream_grad = total.astype(jnp.bfloat16)
    dweight = jnp.einsum('tjc,tjd->cd', dlin, hidden, precision=lax.Precision.HIGHEST)
    proj_grad = gain[None, :] * dweight / jnp.sqrt(4.0 * TOKENS * D)
    gain_grad = lax.optimization_barrier(jnp.sum(dweight * projection, axis=0)) / jnp.sqrt(4.0 * TOKENS)
    return (stream_grad, out_grad, proj_grad, gain_grad)
```

```python
import jax
import jax.numpy as jnp
from jax import lax
from jax.experimental import pallas as pl
from jax.experimental.pallas import tpu as pltpu
from jax.sharding import PartitionSpec as P

F32 = jnp.float32
BF16 = jnp.bfloat16
HIGHEST = lax.Precision.HIGHEST
COLUMNS = 6
PAD = 8
QUARTERS = 4
STAT_TOKENS = 32
MIX_TOKENS = 16
VMEM_LIMIT = 30 * 1024 * 1024


def dot(a, b, dims, precision=None):
    return lax.dot_general(a, b, ((dims[0:1], dims[1:2]), ((), ())), precision=precision, preferred_element_type=F32)


def iota(shape, axis):
    return lax.broadcasted_iota(jnp.int32, shape, axis)


def split(value):
    high = value.astype(BF16)
    return high, (value - high.astype(F32)).astype(BF16)


def select_rows(shape, rows):
    row, lane = iota(shape, 0), iota(shape, 1)
    picked = jnp.zeros(shape, jnp.bool_)
    for index, first, count, step in rows:
        inside = (row == index) & (lane >= first) & (lane < first + count)
        picked = picked | (inside & ((lane - first) % step == 0))
    return picked.astype(F32)


def statistics(h_ref, g_ref, y_ref, g0_ref, gain_ref, proj_ref, stat_ref, hr_ref, gr_ref, w_ref):
    tokens, streams, width = h_ref.shape
    rows = tokens * streams

    @pl.when(pl.program_id(0) == 0)
    def _():
        high, low = split(gain_ref[...] * proj_ref[...])
        none = jnp.zeros((PAD - COLUMNS, width), F32)
        w_ref[...] = jnp.concatenate([high.astype(F32), none, low.astype(F32), none], axis=0).astype(BF16)

    own = pl.ds(pl.multiple_of(pl.program_id(0) * rows, rows), rows)
    h = h_ref[...].reshape(rows, width)
    g = g_ref[...].reshape(rows, width)
    hr_ref[own, :] = h
    gr_ref[own, :] = g
    left = jnp.concatenate([h, g], axis=0)
    right = jnp.concatenate([g, g0_ref[...], w_ref[...], y_ref[...]], axis=0)
    product = dot(left, right, (1, 1))
    at_g0, at_w, at_y, end = rows, rows + tokens, rows + tokens + 2 * PAD, rows + 2 * tokens + 2 * PAD
    token, lane = iota((rows, end), 0) // streams, iota((rows, end), 1)
    of_h = ((lane < at_g0) & (lane // streams == token)) | (lane - at_g0 == token) | ((lane >= at_w) & (lane < at_y))
    of_g = lane - at_y == token
    picked = jnp.where(of_h, product[:rows], 0.0) + jnp.where(of_g, product[rows:], 0.0)
    gather = [(0, at_y, tokens, 1), (1, at_g0, tokens, 1)]
    gather += [(2 + k, k, rows - k, streams) for k in range(streams)]
    gather += [(PAD + c, at_w + c, PAD + 1, PAD) for c in range(COLUMNS)]
    stat = dot(select_rows((2 * PAD, end), gather), picked, (1, 1), HIGHEST)
    lanes = 128
    square = jnp.zeros((rows, lanes), F32)
    for start in range(0, width, lanes):
        part = h[:, start : start + lanes].astype(F32)
        square = square + part * part
    stat_ref[...] = stat + dot(select_rows((2 * PAD, lanes), [(COLUMNS, 0, lanes, 1)]), square, (1, 1), HIGHEST)


def scales_of(scale_ref, shape):
    row = iota(shape, 0)
    return jnp.where(row == 0, scale_ref[0], jnp.where(row == 1, scale_ref[1], scale_ref[2]))


def partials(full_width, *refs):
    *stat_refs, scale_ref, hr_ref, coef_ref, dw_ref = refs
    total = stat_refs[0][...]
    for ref in stat_refs[1:]:
        total = total + ref[...]
    dcoef, lin = total[:PAD], total[PAD:]
    square = dcoef[COLUMNS : COLUMNS + 1]
    inv_rms = lax.rsqrt(square / full_width + 1e-06)
    bent = jnp.tanh(inv_rms * lin)
    scales = scales_of(scale_ref, bent.shape)
    dpre = jnp.where(iota(bent.shape, 0) < COLUMNS, dcoef * scales * (1.0 - bent * bent), 0.0)
    dlin = dpre * inv_rms
    dsquare = -0.5 * inv_rms * inv_rms * inv_rms / full_width * jnp.sum(dpre * lin, axis=0, keepdims=True)
    high, low = split(dlin)
    left = jnp.concatenate([high.astype(F32), low.astype(F32)], axis=0).astype(BF16)
    coef_ref[0:PAD] = scales * bent
    coef_ref[PAD : 2 * PAD] = dlin
    coef_ref[2 * PAD : 3 * PAD] = jnp.broadcast_to(2.0 * dsquare, bent.shape)
    both = dot(left, hr_ref[...], (1, 0))
    dw = both[:PAD] + both[PAD:]
    part = dw.shape[1] // QUARTERS
    for q in range(QUARTERS):
        dw_ref[q * COLUMNS : (q + 1) * COLUMNS, :] = dw[:COLUMNS, q * part : (q + 1) * part]


def outputs(coef_ref, mix_ref, hr_ref, gr_ref, g0_ref, w_ref, *refs):
    grad_ref, out_ref = refs[-2:]
    tokens, streams, width = grad_ref.shape
    coef = coef_ref[...]
    bent = coef[:PAD]
    row, stream = iota(bent.shape, 0), iota(bent.shape, 1) % streams
    static = jnp.zeros(bent.shape, F32)
    for j in range(streams):
        for c in range(COLUMNS):
            static = jnp.where((row == c) & (stream == j), mix_ref[j, c], static)
    coef = jnp.concatenate([static + bent, coef[PAD:]], axis=0)
    group = min(MIX_TOKENS, tokens)
    rows = group * streams
    at_g0, at_w, at_h, end = rows, rows + group, rows + group + 2 * PAD, 2 * rows + group + 2 * PAD
    spread = [(1, at_g0, group, 1), (2 * PAD, at_h, rows, 1)]
    spread += [(2 + k, k, rows - k, streams) for k in range(streams)]
    spread += [(PAD + c, at_w + c, PAD + 1, PAD) for c in range(COLUMNS)]
    spread = select_rows((3 * PAD, end), spread)
    token, line, lane = iota((rows, end), 0) // streams, iota((rows, end), 0), iota((rows, end), 1)
    kept = ((lane < at_g0) & (lane // streams == token)) | (lane - at_g0 == token) | (lane - at_h == line)
    kept = kept | ((lane >= at_w) & (lane < at_h))
    out_token, out_lane = iota((group, end), 0), iota((group, end), 1)
    out_kept = (out_lane < at_g0) & (out_lane // streams == out_token)
    step = min(width, 1024)
    for start in range(0, tokens, group):
        here = coef[:, start * streams : start * streams + rows]
        high, low = split(jnp.where(kept, dot(here, spread, (0, 0), HIGHEST), 0.0))
        beta = jnp.concatenate([here[0:1], jnp.zeros((1, end - rows), F32)], axis=1)
        out_high, out_low = split(jnp.where(out_kept, jnp.broadcast_to(beta, (group, end)), 0.0))
        left = jnp.concatenate([high, low, out_high, out_low], axis=0)
        own = pl.ds(start * streams, rows)
        for column in range(0, width, step):
            at = pl.ds(column, step)
            right = jnp.concatenate(
                [gr_ref[own, at], g0_ref[start : start + group, at], w_ref[:, at], hr_ref[own, at]], axis=0
            )
            result = dot(left, right, (1, 0))
            total = result[:rows] + result[rows : 2 * rows]
            grad_ref[start : start + group, :, at] = total.astype(BF16).reshape(group, streams, step)
            out_ref[start : start + group, at] = (
                result[2 * rows : 2 * rows + group] + result[2 * rows + group :]
            ).astype(BF16)


def whole(*shape):
    return pl.BlockSpec(shape, lambda *_: (0,) * len(shape))


def shards(streams, layer_out, cotangent, input_cot, gain, projection, static_mix, tanh_scale):
    tokens, count, width = streams.shape
    rows = tokens * count
    dp, tensor = lax.axis_size("dp"), lax.axis_size("tensor")
    full_width = width * tensor
    params = pltpu.CompilerParams(vmem_limit_bytes=VMEM_LIMIT)
    scalars = pl.BlockSpec(memory_space=pltpu.SMEM)

    block = min(STAT_TOKENS, tokens)
    def in_hbm(array):
        return pltpu.with_memory_space_constraint(array, pltpu.HBM)

    streams, cotangent, layer_out, input_cot = map(in_hbm, (streams, cotangent, layer_out, input_cot))
    wide = pl.BlockSpec((block, count, width), lambda i: (i, 0, 0))
    flat = pl.BlockSpec((block, width), lambda i: (i, 0))
    stat, hr, gr, w = pl.pallas_call(
        statistics,
        grid=(tokens // block,),
        in_specs=[wide, wide, flat, flat, whole(1, width), whole(COLUMNS, width)],
        out_specs=[
            pl.BlockSpec((2 * PAD, block * count), lambda i: (0, i)),
            whole(rows, width),
            whole(rows, width),
            whole(2 * PAD, width),
        ],
        out_shape=[
            jax.ShapeDtypeStruct((2 * PAD, rows), F32),
            jax.ShapeDtypeStruct((rows, width), BF16),
            jax.ShapeDtypeStruct((rows, width), BF16),
            jax.ShapeDtypeStruct((2 * PAD, width), BF16),
        ],
        compiler_params=params,
        name="statistics",
    )(streams, cotangent, layer_out, input_cot, in_hbm(gain.reshape(1, width)), in_hbm(projection))

    if tensor == 2:
        stats = (stat, lax.ppermute(stat, "tensor", [(0, 1), (1, 0)]))
    else:
        stats = (lax.psum(stat, "tensor"),)

    coef, dw = pl.pallas_call(
        lambda *refs: partials(float(full_width), *refs),
        in_specs=[pl.BlockSpec(memory_space=pltpu.VMEM)] * len(stats) + [scalars, pl.BlockSpec(memory_space=pltpu.VMEM)],
        out_specs=[pl.BlockSpec(memory_space=pltpu.VMEM)] * 2,
        out_shape=[
            jax.ShapeDtypeStruct((3 * PAD, rows), F32),
            jax.ShapeDtypeStruct((QUARTERS * COLUMNS, width // QUARTERS), F32),
        ],
        compiler_params=params,
        name="partials",
    )(*stats, tanh_scale, hr)

    def mixed(index, previous):
        wide_at = pl.BlockSpec((block, count, width), lambda i: (index, 0, 0))
        flat_at = pl.BlockSpec((block, width), lambda i: (index, 0))
        lines = pl.BlockSpec((block * count, width), lambda i: (index, 0))
        return pl.pallas_call(
            outputs,
            grid=(1,),
            in_specs=[
                pl.BlockSpec((3 * PAD, block * count), lambda i: (0, index)),
                scalars,
                lines,
                lines,
                flat_at,
                whole(2 * PAD, width),
            ]
            + [pl.BlockSpec(memory_space=pl.ANY)] * len(previous),
            out_specs=[wide_at, flat_at],
            out_shape=[
                jax.ShapeDtypeStruct((tokens, count, width), BF16),
                jax.ShapeDtypeStruct((tokens, width), BF16),
            ],
            input_output_aliases={6 + i: i for i in range(len(previous))},
            compiler_params=params,
            cost_estimate=pl.CostEstimate(flops=4_000_000_000, bytes_accessed=block * width * 30, transcendentals=0),
            name="outputs",
        )(coef, static_mix, hr, gr, input_cot, w, *previous)

    grads = ()
    for index in range(tokens // block):
        grads = mixed(index, grads)
    stream_grad, out_grad = grads

    if dp & (dp - 1) == 0:
        step = 1
        while step < dp:
            dw = dw + lax.ppermute(dw, "dp", [(i, i ^ step) for i in range(dp)])
            step *= 2
    else:
        dw = lax.psum(dw, "dp")
    part = width // QUARTERS
    dw = jnp.concatenate([dw[q * COLUMNS : (q + 1) * COLUMNS] for q in range(QUARTERS)], axis=1)
    all_tokens = tokens * dp
    proj_grad = gain[None, :] * dw / jnp.sqrt(float(count) * all_tokens * full_width)
    gain_grad = jnp.sum(dw * projection, axis=0) / jnp.sqrt(float(count) * all_tokens)
    return (stream_grad, out_grad, proj_grad, gain_grad)


def solution(mesh):
    placed = (
        P("dp", None, "tensor"),
        P("dp", "tensor"),
        P("dp", None, "tensor"),
        P("dp", "tensor"),
        P("tensor"),
        P(None, "tensor"),
        P(),
        P(),
    )
    return jax.shard_map(
        shards,
        mesh=mesh,
        in_specs=placed,
        out_specs=(P("dp", None, "tensor"), P("dp", "tensor"), P(None, "tensor"), P("tensor")),
        check_vma=False,
    )
```

```python
import jax
import jax.numpy as jnp
from jax import lax
from jax.experimental import pallas as pl
from jax.experimental.pallas import tpu as pltpu
from jax.sharding import PartitionSpec as P

F32 = jnp.float32
BF16 = jnp.bfloat16
HIGHEST = lax.Precision.HIGHEST
COLUMNS = 6
PAD = 8
QUARTERS = 4
STAT_TOKENS = 32
MIX_TOKENS = 16
WINDOWS = 4
AHEAD = 2
VMEM_LIMIT = 30 * 1024 * 1024


def dot(a, b, dims, precision=None):
    return lax.dot_general(a, b, ((dims[0:1], dims[1:2]), ((), ())), precision=precision, preferred_element_type=F32)


def iota(shape, axis):
    return lax.broadcasted_iota(jnp.int32, shape, axis)


def split(value):
    high = value.astype(BF16)
    return high, (value - high.astype(F32)).astype(BF16)


def select_rows(shape, rows):
    row, lane = iota(shape, 0), iota(shape, 1)
    picked = jnp.zeros(shape, jnp.bool_)
    for index, first, count, step in rows:
        inside = (row == index) & (lane >= first) & (lane < first + count)
        picked = picked | (inside & ((lane - first) % step == 0))
    return picked.astype(F32)


def statistics(
    h_hbm, g_hbm, y_hbm, g0_hbm, gain_hbm, proj_hbm, stat_ref, hr_ref, gr_ref, g0_ref, w_ref, h_buf, g_buf, y_buf, gain_buf, proj_buf, sems, more_sems
):
    total, streams, width = h_hbm.shape
    blocks = sems.shape[0]
    tokens = total // blocks
    weights = [
        pltpu.make_async_copy(gain_hbm, gain_buf, more_sems.at[0]),
        pltpu.make_async_copy(proj_hbm, proj_buf, more_sems.at[1]),
    ]

    def copies(block):
        at = pl.ds(pl.multiple_of(block * tokens, tokens), tokens)
        pairs = [(h_hbm, h_buf), (g_hbm, g_buf), (g0_hbm, g0_ref), (y_hbm, y_buf)]
        return [
            pltpu.make_async_copy(source.at[at], target.at[at], sems.at[block, index])
            for index, (source, target) in enumerate(pairs)
        ]

    for copy in weights:
        copy.start()
    for block in range(min(AHEAD, blocks)):
        for copy in copies(block):
            copy.start(priority=block % 2)
    for copy in weights:
        copy.wait()
    high, low = split(gain_buf[...] * proj_buf[...])
    none = jnp.zeros((PAD - COLUMNS, width), F32)
    w_ref[...] = jnp.concatenate([high.astype(F32), none, low.astype(F32), none], axis=0).astype(BF16)

    @pl.loop(0, blocks)
    def _(block):
        for copy in copies(block):
            copy.wait()

        @pl.when(block + AHEAD < blocks)
        def _():
            for copy in copies(block + AHEAD):
                copy.start(priority=1)

        statistics_of(block, tokens, stat_ref, hr_ref, gr_ref, g0_ref, w_ref, h_buf, g_buf, y_buf)


def statistics_of(block, tokens, stat_ref, hr_ref, gr_ref, g0_ref, w_ref, h_buf, g_buf, y_buf):
    _, streams, width = h_buf.shape
    rows = tokens * streams
    at = pl.ds(pl.multiple_of(block * tokens, tokens), tokens)
    own = pl.ds(pl.multiple_of(block * rows, rows), rows)
    hr_ref[own, :] = h_buf[at].reshape(rows, width)
    gr_ref[own, :] = g_buf[at].reshape(rows, width)
    h = hr_ref[own, :]
    left = jnp.concatenate([gr_ref[own, :], g0_ref[at, :], w_ref[...]], axis=0)
    product = dot(left, jnp.concatenate([h, y_buf[at, :]], axis=0), (1, 1))
    lanes = 128
    square = jnp.zeros((rows, lanes), F32)
    for start in range(0, width, lanes):
        part = h[:, start : start + lanes].astype(F32)
        square = square + part * part
    square = jnp.sum(square.T, axis=0, keepdims=True)
    line, token = iota((rows, rows), 0), iota((rows, rows), 1) // streams
    mixer = jnp.where(line // streams == token, product[:rows, :rows], 0.0)
    mixer = jnp.sum(mixer.reshape(rows // PAD, PAD, rows), axis=0)
    folded = mixer[:streams]
    for start in range(streams, PAD, streams):
        folded = folded + mixer[start : start + streams]
    alpha = jnp.where(line[:tokens] == token[:tokens], product[rows : rows + tokens, :rows], 0.0)
    alpha = jnp.sum(alpha, axis=0, keepdims=True)
    beta = jnp.where(line[:tokens] == token[:tokens], product[:rows, rows:].T, 0.0)
    beta = jnp.sum(beta, axis=0, keepdims=True)
    lin = product[rows + tokens : rows + tokens + PAD, :rows] + product[rows + tokens + PAD :, :rows]
    stat_ref[:, own] = jnp.concatenate([beta, alpha, folded, square, jnp.zeros_like(square), lin], axis=0)


def scales_of(scale_ref, shape):
    row = iota(shape, 0)
    return jnp.where(row == 0, scale_ref[0], jnp.where(row == 1, scale_ref[1], scale_ref[2]))


def partials(full_width, *refs):
    *stat_refs, scale_ref, hr_ref, coef_ref, dw_ref = refs
    total = stat_refs[0][...]
    for ref in stat_refs[1:]:
        total = total + ref[...]
    dcoef, lin = total[:PAD], total[PAD:]
    square = dcoef[COLUMNS : COLUMNS + 1]
    inv_rms = lax.rsqrt(square / full_width + 1e-06)
    bent = jnp.tanh(inv_rms * lin)
    scales = scales_of(scale_ref, bent.shape)
    dpre = jnp.where(iota(bent.shape, 0) < COLUMNS, dcoef * scales * (1.0 - bent * bent), 0.0)
    dlin = dpre * inv_rms
    dsquare = -0.5 * inv_rms * inv_rms * inv_rms / full_width * jnp.sum(dpre * lin, axis=0, keepdims=True)
    high, low = split(dlin)
    left = jnp.concatenate([high.astype(F32), low.astype(F32)], axis=0).astype(BF16)
    coef = jnp.concatenate([scales * bent, dlin, jnp.broadcast_to(2.0 * dsquare, bent.shape)], axis=0)
    groups, _, lanes = coef_ref.shape
    for index in range(groups):
        coef_ref[index] = coef[:, index * lanes : (index + 1) * lanes]
    both = dot(left, hr_ref[...], (1, 0))
    dw = both[:PAD] + both[PAD:]
    part = dw.shape[1] // QUARTERS
    for q in range(QUARTERS):
        dw_ref[q * COLUMNS : (q + 1) * COLUMNS, :] = dw[:COLUMNS, q * part : (q + 1) * part]


def put(refs, first, sems):
    grad_buf, out_buf, grad_hbm, out_hbm = refs
    at = pl.ds(first, out_buf.shape[0])
    return [
        pltpu.make_async_copy(grad_buf, grad_hbm.at[at], sems.at[0]),
        pltpu.make_async_copy(out_buf, out_hbm.at[at], sems.at[1]),
    ]


def outputs(first, groups, finished, last, coef_ref, mix_ref, hr_ref, gr_ref, g0_ref, w_ref, *refs):
    *results, grad_buf, out_buf, sems, more_sems = refs
    group, streams, width = grad_buf.shape[0] // groups, grad_buf.shape[1], grad_buf.shape[2]
    copies = put((*refs[:2], *results[-2:]), first * group - refs[1].shape[0], sems) if finished else []
    for copy in copies:
        copy.start()
    rows = group * streams
    at_g0, at_w, at_h, end = rows, rows + group, rows + group + 2 * PAD, 2 * rows + group + 2 * PAD
    spread = [(1, at_g0, group, 1), (2 * PAD, at_h, rows, 1)]
    spread += [(2 + k, k, rows - k, streams) for k in range(streams)]
    spread += [(PAD + c, at_w + c, PAD + 1, PAD) for c in range(COLUMNS)]
    spread = select_rows((3 * PAD, end), spread)
    token, line, lane = iota((rows, end), 0) // streams, iota((rows, end), 0), iota((rows, end), 1)
    kept = ((lane < at_g0) & (lane // streams == token)) | (lane - at_g0 == token) | (lane - at_h == line)
    kept = kept | ((lane >= at_w) & (lane < at_h))
    out_token, out_lane = iota((group, end), 0), iota((group, end), 1)
    out_kept = (out_lane < at_g0) & (out_lane // streams == out_token)
    row, stream = iota((PAD, rows), 0), iota((PAD, rows), 1) % streams
    static = jnp.zeros((PAD, rows), F32)
    for j in range(streams):
        for c in range(COLUMNS):
            static = jnp.where((row == c) & (stream == j), mix_ref[j, c], static)
    lefts = []
    for index in range(groups):
        here = coef_ref[first + index]
        here = jnp.concatenate([static + here[:PAD], here[PAD:]], axis=0)
        high, low = split(jnp.where(kept, dot(here, spread, (0, 0), HIGHEST), 0.0))
        beta = jnp.concatenate([here[0:1], jnp.zeros((1, end - rows), F32)], axis=1)
        out_high, out_low = split(jnp.where(out_kept, jnp.broadcast_to(beta, (group, end)), 0.0))
        lefts.append(jnp.concatenate([high, low, out_high, out_low], axis=0))
    step = min(width, 1024)
    for index, left in enumerate(lefts):
        own = pl.ds((first + index) * rows, rows)
        source = pl.ds((first + index) * group, group)
        target = pl.ds(index * group, group)
        for column in range(0, width, step):
            at = pl.ds(column, step)
            right = jnp.concatenate([gr_ref[own, at], g0_ref[source, at], w_ref[:, at], hr_ref[own, at]], axis=0)
            result = dot(left, right, (1, 0))
            total = result[:rows] + result[rows : 2 * rows]
            grad_buf[target, :, at] = total.astype(BF16).reshape(group, streams, step)
            out_buf[target, at] = (result[2 * rows : 2 * rows + group] + result[2 * rows + group :]).astype(BF16)
    if last:
        own = put((grad_buf, out_buf, *results[-2:]), first * group, more_sems)
        for copy in own:
            copy.start()
        copies += own
    for copy in copies:
        copy.wait()


def tail(proj_scale, gain_scale, dw_ref, more_ref, gain_ref, proj_ref, proj_grad_ref, gain_grad_ref):
    dw = dw_ref[...] + more_ref[...]
    part = dw.shape[1]
    for q in range(QUARTERS):
        at = pl.ds(q * part, part)
        own = dw[q * COLUMNS : (q + 1) * COLUMNS]
        proj_grad_ref[:, at] = gain_ref[:, at] * own * proj_scale
        gain_grad_ref[:, at] = jnp.sum(own * proj_ref[:, at], axis=0, keepdims=True) * gain_scale


def step_orders(devices):
    steps = [1 << bit for bit in range(devices.bit_length() - 1)]
    half = len(steps) // 2
    even, odd = [], []
    for near, far in zip(steps[:half], steps[half:]):
        even += [near, far]
        odd += [far, near]
    return even + steps[2 * half :], odd + steps[2 * half :]


def shards(streams, layer_out, cotangent, input_cot, gain, projection, static_mix, tanh_scale):
    tokens, count, width = streams.shape
    rows = tokens * count
    dp, tensor = lax.axis_size("dp"), lax.axis_size("tensor")
    full_width = width * tensor
    params = pltpu.CompilerParams(vmem_limit_bytes=VMEM_LIMIT)
    scalars = pl.BlockSpec(memory_space=pltpu.SMEM)

    block = min(STAT_TOKENS, tokens)
    def in_hbm(array):
        return pltpu.with_memory_space_constraint(array, pltpu.HBM)

    def in_vmem(array):
        return pltpu.with_memory_space_constraint(array, pltpu.VMEM)

    streams, cotangent, layer_out, input_cot = map(in_hbm, (streams, cotangent, layer_out, input_cot))
    vmem = pl.BlockSpec(memory_space=pltpu.VMEM)
    hbm = pl.BlockSpec(memory_space=pltpu.HBM)
    stat, hr, gr, g0, w = pl.pallas_call(
        statistics,
        in_specs=[hbm] * 6,
        out_specs=[vmem] * 5,
        out_shape=[
            pltpu.VMEM((2 * PAD, rows), F32),
            pltpu.VMEM((rows, width), BF16),
            pltpu.VMEM((rows, width), BF16),
            pltpu.VMEM((tokens, width), BF16),
            pltpu.VMEM((2 * PAD, width), BF16),
        ],
        scratch_shapes=[
            pltpu.VMEM(streams.shape, BF16),
            pltpu.VMEM(streams.shape, BF16),
            pltpu.VMEM(layer_out.shape, BF16),
            pltpu.VMEM((1, width), F32),
            pltpu.VMEM((COLUMNS, width), F32),
            pltpu.SemaphoreType.DMA((tokens // block, 4)),
            pltpu.SemaphoreType.DMA((2,)),
        ],
        compiler_params=params,
        name="statistics",
    )(streams, cotangent, layer_out, input_cot, in_hbm(gain.reshape(1, width)), in_hbm(projection))

    if tensor == 2:
        stats = (stat, lax.ppermute(stat, "tensor", [(0, 1), (1, 0)]))
    else:
        stats = (lax.psum(stat, "tensor"),)

    group = min(MIX_TOKENS, tokens)
    coef, dw = pl.pallas_call(
        lambda *refs: partials(float(full_width), *refs),
        in_specs=[vmem] * len(stats) + [scalars, vmem],
        out_specs=[vmem] * 2,
        out_shape=[
            pltpu.VMEM((tokens // group, 3 * PAD, group * count), F32),
            pltpu.VMEM((QUARTERS * COLUMNS, width // QUARTERS), F32),
        ],
        compiler_params=params,
        name="partials",
    )(*stats, tanh_scale, in_vmem(hr))

    grads = [jax.ShapeDtypeStruct((tokens, count, width), BF16), jax.ShapeDtypeStruct((tokens, width), BF16)]

    def mixed(first, groups, last, bufs, results):
        own = groups * group
        kept = [pltpu.VMEM((own, count, width), BF16), pltpu.VMEM((own, width), BF16)]
        sems = [pltpu.SemaphoreType.DMA((2,))] * 2
        shape = (grads if bufs or last else []) + ([] if last else kept)
        done = pl.pallas_call(
            lambda *refs: outputs(first, groups, bool(bufs), last, *refs),
            in_specs=[vmem, scalars] + [vmem] * (4 + len(bufs)) + [hbm] * len(results),
            out_specs=([hbm] * 2 if bufs or last else []) + ([] if last else [vmem] * 2),
            out_shape=shape,
            scratch_shapes=(kept if last else []) + sems,
            input_output_aliases={8 + i: i for i in range(len(results))},
            compiler_params=params,
            cost_estimate=pl.CostEstimate(flops=4_000_000_000, bytes_accessed=own * width * 30, transcendentals=0),
            name="outputs",
        )(in_vmem(coef), static_mix, *map(in_vmem, (hr, gr, g0, w, *bufs)), *results)
        return ((), done) if last else (done[-2:], done[:-2])

    sizes = [tokens // group]
    if sizes[0] % WINDOWS == 0 and sizes[0] > WINDOWS:
        each = sizes[0] // WINDOWS
        sizes = [each + 1] + [each] * (WINDOWS - 2) + [each - 1]
    bufs, results, first = (), (), 0
    for index, groups in enumerate(sizes):
        bufs, results = mixed(first, groups, index == len(sizes) - 1, bufs, results)
        first += groups
    stream_grad, out_grad = results

    if dp > 1 and dp & (dp - 1) == 0:
        orders = step_orders(dp)
        for index in range(len(orders[0])):
            pairs = [
                (i * tensor + t, (i ^ orders[t % 2][index]) * tensor + t) for i in range(dp) for t in range(tensor)
            ]
            more = lax.ppermute(dw, ("dp", "tensor"), pairs)
            if index < len(orders[0]) - 1:
                dw = dw + more
    else:
        dw, more = lax.psum(dw, "dp"), jnp.zeros_like(dw)
    all_tokens = tokens * dp
    proj_scale = (float(count) * all_tokens * full_width) ** -0.5
    gain_scale = (float(count) * all_tokens) ** -0.5
    proj_grad, gain_grad = pl.pallas_call(
        lambda *refs: tail(proj_scale, gain_scale, *refs),
        in_specs=[vmem] * 4,
        out_specs=[vmem] * 2,
        out_shape=[jax.ShapeDtypeStruct((COLUMNS, width), F32), jax.ShapeDtypeStruct((1, width), F32)],
        compiler_params=params,
        name="tail",
    )(dw, more, gain.reshape(1, width), projection)
    return (stream_grad, out_grad, proj_grad, gain_grad.reshape(width))


def solution(mesh):
    placed = (
        P("dp", None, "tensor"),
        P("dp", "tensor"),
        P("dp", None, "tensor"),
        P("dp", "tensor"),
        P("tensor"),
        P(None, "tensor"),
        P(),
        P(),
    )
    return jax.shard_map(
        shards,
        mesh=mesh,
        in_specs=placed,
        out_specs=(P("dp", None, "tensor"), P("dp", "tensor"), P(None, "tensor"), P("tensor")),
        check_vma=False,
    )
```

```python
import jax
import jax.numpy as jnp
from jax import lax
from jax.experimental import pallas as pl
from jax.experimental.pallas import tpu as pltpu
from jax.sharding import PartitionSpec as P

F32 = jnp.float32
BF16 = jnp.bfloat16
HIGHEST = lax.Precision.HIGHEST
COLUMNS = 6
PAD = 8
QUARTERS = 4
STAT_TOKENS = 32
MIX_TOKENS = 16
WINDOWS = 4
DEPTHS = 4
VMEM_LIMIT = 30 * 1024 * 1024


def dot(a, b, dims, precision=None):
    return lax.dot_general(a, b, ((dims[0:1], dims[1:2]), ((), ())), precision=precision, preferred_element_type=F32)


def iota(shape, axis):
    return lax.broadcasted_iota(jnp.int32, shape, axis)


def split(value):
    high = value.astype(BF16)
    return high, (value - high.astype(F32)).astype(BF16)


def select_rows(shape, rows):
    row, lane = iota(shape, 0), iota(shape, 1)
    picked = jnp.zeros(shape, jnp.bool_)
    for index, first, count, step in rows:
        inside = (row == index) & (lane >= first) & (lane < first + count)
        picked = picked | (inside & ((lane - first) % step == 0))
    return picked.astype(F32)


def statistics(
    h_hbm, g_hbm, y_hbm, g0_hbm, gain_hbm, proj_hbm, stat_ref, hr_ref, gr_ref, g0_ref, w_ref, h_buf, g_buf, y_buf, gain_buf, proj_buf, sems, more_sems
):
    total, streams, width = h_hbm.shape
    blocks = sems.shape[0]
    tokens = total // blocks
    weights = [
        pltpu.make_async_copy(gain_hbm, gain_buf, more_sems.at[0]),
        pltpu.make_async_copy(proj_hbm, proj_buf, more_sems.at[1]),
    ]

    def copies(block):
        at = pl.ds(pl.multiple_of(block * tokens, tokens), tokens)
        pairs = [(h_hbm, h_buf), (g_hbm, g_buf), (g0_hbm, g0_ref), (y_hbm, y_buf)]
        return [
            pltpu.make_async_copy(source.at[at], target.at[at], sems.at[block, index])
            for index, (source, target) in enumerate(pairs)
        ]

    for copy in weights:
        copy.start()
    for block in range(blocks):
        for copy in copies(block):
            copy.start(priority=min(block, 1))
    for copy in weights:
        copy.wait()
    high, low = split(gain_buf[...] * proj_buf[...])
    none = jnp.zeros((PAD - COLUMNS, width), F32)
    w_ref[...] = jnp.concatenate([high.astype(F32), none, low.astype(F32), none], axis=0).astype(BF16)

    @pl.loop(0, blocks)
    def _(block):
        for copy in copies(block):
            copy.wait()

        statistics_of(block, tokens, stat_ref, hr_ref, gr_ref, g0_ref, w_ref, h_buf, g_buf, y_buf)


def statistics_of(block, tokens, stat_ref, hr_ref, gr_ref, g0_ref, w_ref, h_buf, g_buf, y_buf):
    _, streams, width = h_buf.shape
    rows = tokens * streams
    at = pl.ds(pl.multiple_of(block * tokens, tokens), tokens)
    own = pl.ds(pl.multiple_of(block * rows, rows), rows)
    product = 0.0
    depth = width // DEPTHS
    for start in range(0, width, depth):
        part = pl.ds(start, depth)
        hr_ref[own, part] = h_buf[at, :, part].reshape(rows, depth)
        gr_ref[own, part] = g_buf[at, :, part].reshape(rows, depth)
        left = jnp.concatenate([gr_ref[own, part], g0_ref[at, part], w_ref[:, part]], axis=0)
        product = product + dot(left, jnp.concatenate([hr_ref[own, part], y_buf[at, part]], axis=0), (1, 1))
    lanes = 128
    square = jnp.zeros((rows, lanes), F32)
    for start in range(0, width, lanes):
        part = hr_ref[own, pl.ds(start, lanes)].astype(F32)
        square = square + part * part
    square = jnp.sum(square.T, axis=0, keepdims=True)
    line, token = iota((rows, rows), 0), iota((rows, rows), 1) // streams
    mixer = jnp.where(line // streams == token, product[:rows, :rows], 0.0)
    mixer = jnp.sum(mixer.reshape(rows // PAD, PAD, rows), axis=0)
    folded = mixer[:streams]
    for start in range(streams, PAD, streams):
        folded = folded + mixer[start : start + streams]
    alpha = jnp.where(line[:tokens] == token[:tokens], product[rows : rows + tokens, :rows], 0.0)
    alpha = jnp.sum(alpha, axis=0, keepdims=True)
    beta = jnp.where(line[:tokens] == token[:tokens], product[:rows, rows:].T, 0.0)
    beta = jnp.sum(beta, axis=0, keepdims=True)
    lin = product[rows + tokens : rows + tokens + PAD, :rows] + product[rows + tokens + PAD :, :rows]
    stat_ref[:, own] = jnp.concatenate([beta, alpha, folded, square, jnp.zeros_like(square), lin], axis=0)


def scales_of(scale_ref, shape):
    row = iota(shape, 0)
    return jnp.where(row == 0, scale_ref[0], jnp.where(row == 1, scale_ref[1], scale_ref[2]))


def partials(full_width, *refs):
    *stat_refs, scale_ref, hr_ref, coef_ref, dw_ref = refs
    total = stat_refs[0][...]
    for ref in stat_refs[1:]:
        total = total + ref[...]
    dcoef, lin = total[:PAD], total[PAD:]
    square = dcoef[COLUMNS : COLUMNS + 1]
    inv_rms = lax.rsqrt(square / full_width + 1e-06)
    bent = jnp.tanh(inv_rms * lin)
    scales = scales_of(scale_ref, bent.shape)
    dpre = jnp.where(iota(bent.shape, 0) < COLUMNS, dcoef * scales * (1.0 - bent * bent), 0.0)
    dlin = dpre * inv_rms
    dsquare = -0.5 * inv_rms * inv_rms * inv_rms / full_width * jnp.sum(dpre * lin, axis=0, keepdims=True)
    high, low = split(dlin)
    left = jnp.concatenate([high.astype(F32), low.astype(F32)], axis=0).astype(BF16)
    coef = jnp.concatenate([scales * bent, dlin, jnp.broadcast_to(2.0 * dsquare, bent.shape)], axis=0)
    groups, _, lanes = coef_ref.shape
    for index in range(groups):
        coef_ref[index] = coef[:, index * lanes : (index + 1) * lanes]
    both = dot(left, hr_ref[...], (1, 0))
    dw = both[:PAD] + both[PAD:]
    part = dw.shape[1] // QUARTERS
    for q in range(QUARTERS):
        dw_ref[q * COLUMNS : (q + 1) * COLUMNS, :] = dw[:COLUMNS, q * part : (q + 1) * part]


def put(refs, first, sems):
    grad_buf, out_buf, grad_hbm, out_hbm = refs
    at = pl.ds(first, out_buf.shape[0])
    return [
        pltpu.make_async_copy(grad_buf, grad_hbm.at[at], sems.at[0]),
        pltpu.make_async_copy(out_buf, out_hbm.at[at], sems.at[1]),
    ]


def outputs(first, groups, finished, last, coef_ref, mix_ref, hr_ref, gr_ref, g0_ref, w_ref, *refs):
    *results, grad_buf, out_buf, sems, more_sems = refs
    group, streams, width = grad_buf.shape[0] // groups, grad_buf.shape[1], grad_buf.shape[2]
    copies = put((*refs[:2], *results[-2:]), first * group - refs[1].shape[0], sems) if finished else []
    for copy in copies:
        copy.start()
    rows = group * streams
    at_g0, at_w, at_h, end = rows, rows + group, rows + group + 2 * PAD, 2 * rows + group + 2 * PAD
    spread = [(1, at_g0, group, 1), (2 * PAD, at_h, rows, 1)]
    spread += [(2 + k, k, rows - k, streams) for k in range(streams)]
    spread += [(PAD + c, at_w + c, PAD + 1, PAD) for c in range(COLUMNS)]
    spread = select_rows((3 * PAD, end), spread)
    token, line, lane = iota((rows, end), 0) // streams, iota((rows, end), 0), iota((rows, end), 1)
    kept = ((lane < at_g0) & (lane // streams == token)) | (lane - at_g0 == token) | (lane - at_h == line)
    kept = kept | ((lane >= at_w) & (lane < at_h))
    out_token, out_lane = iota((group, end), 0), iota((group, end), 1)
    out_kept = (out_lane < at_g0) & (out_lane // streams == out_token)
    row, stream = iota((PAD, rows), 0), iota((PAD, rows), 1) % streams
    static = jnp.zeros((PAD, rows), F32)
    for j in range(streams):
        for c in range(COLUMNS):
            static = jnp.where((row == c) & (stream == j), mix_ref[j, c], static)
    lefts = []
    for index in range(groups):
        here = coef_ref[first + index]
        here = jnp.concatenate([static + here[:PAD], here[PAD:]], axis=0)
        high, low = split(jnp.where(kept, dot(here, spread, (0, 0), HIGHEST), 0.0))
        beta = jnp.concatenate([here[0:1], jnp.zeros((1, end - rows), F32)], axis=1)
        out_high, out_low = split(jnp.where(out_kept, jnp.broadcast_to(beta, (group, end)), 0.0))
        lefts.append(jnp.concatenate([high, low, out_high, out_low], axis=0))
    step = min(width, 1024)
    for index, left in enumerate(lefts):
        own = pl.ds((first + index) * rows, rows)
        source = pl.ds((first + index) * group, group)
        target = pl.ds(index * group, group)
        for column in range(0, width, step):
            at = pl.ds(column, step)
            right = jnp.concatenate([gr_ref[own, at], g0_ref[source, at], w_ref[:, at], hr_ref[own, at]], axis=0)
            result = dot(left, right, (1, 0))
            total = result[:rows] + result[rows : 2 * rows]
            grad_buf[target, :, at] = total.astype(BF16).reshape(group, streams, step)
            out_buf[target, at] = (result[2 * rows : 2 * rows + group] + result[2 * rows + group :]).astype(BF16)
    if last:
        own = put((grad_buf, out_buf, *results[-2:]), first * group, more_sems)
        for copy in own:
            copy.start()
        copies += own
    for copy in copies:
        copy.wait()


def tail(proj_scale, gain_scale, dw_ref, more_ref, gain_ref, proj_ref, proj_grad_ref, gain_grad_ref):
    dw = dw_ref[...] + more_ref[...]
    part = dw.shape[1]
    for q in range(QUARTERS):
        at = pl.ds(q * part, part)
        own = dw[q * COLUMNS : (q + 1) * COLUMNS]
        proj_grad_ref[:, at] = gain_ref[:, at] * own * proj_scale
        gain_grad_ref[:, at] = jnp.sum(own * proj_ref[:, at], axis=0, keepdims=True) * gain_scale


def step_orders(devices):
    steps = [1 << bit for bit in range(devices.bit_length() - 1)]
    half = len(steps) // 2
    even, odd = [], []
    for near, far in zip(steps[:half], steps[half:]):
        even += [near, far]
        odd += [far, near]
    return even + steps[2 * half :], odd + steps[2 * half :]


def shards(streams, layer_out, cotangent, input_cot, gain, projection, static_mix, tanh_scale):
    tokens, count, width = streams.shape
    rows = tokens * count
    dp, tensor = lax.axis_size("dp"), lax.axis_size("tensor")
    full_width = width * tensor
    params = pltpu.CompilerParams(vmem_limit_bytes=VMEM_LIMIT)
    scalars = pl.BlockSpec(memory_space=pltpu.SMEM)

    block = min(STAT_TOKENS, tokens)
    def in_hbm(array):
        return pltpu.with_memory_space_constraint(array, pltpu.HBM)

    def in_vmem(array):
        return pltpu.with_memory_space_constraint(array, pltpu.VMEM)

    streams, cotangent, layer_out, input_cot = map(in_hbm, (streams, cotangent, layer_out, input_cot))
    vmem = pl.BlockSpec(memory_space=pltpu.VMEM)
    hbm = pl.BlockSpec(memory_space=pltpu.HBM)
    stat, hr, gr, g0, w = pl.pallas_call(
        statistics,
        in_specs=[hbm] * 6,
        out_specs=[vmem] * 5,
        out_shape=[
            pltpu.VMEM((2 * PAD, rows), F32),
            pltpu.VMEM((rows, width), BF16),
            pltpu.VMEM((rows, width), BF16),
            pltpu.VMEM((tokens, width), BF16),
            pltpu.VMEM((2 * PAD, width), BF16),
        ],
        scratch_shapes=[
            pltpu.VMEM(streams.shape, BF16),
            pltpu.VMEM(streams.shape, BF16),
            pltpu.VMEM(layer_out.shape, BF16),
            pltpu.VMEM((1, width), F32),
            pltpu.VMEM((COLUMNS, width), F32),
            pltpu.SemaphoreType.DMA((tokens // block, 4)),
            pltpu.SemaphoreType.DMA((2,)),
        ],
        compiler_params=params,
        name="statistics",
    )(streams, cotangent, layer_out, input_cot, in_hbm(gain.reshape(1, width)), in_hbm(projection))

    if tensor == 2:
        stats = (stat, lax.ppermute(stat, "tensor", [(0, 1), (1, 0)]))
    else:
        stats = (lax.psum(stat, "tensor"),)

    group = min(MIX_TOKENS, tokens)
    coef, dw = pl.pallas_call(
        lambda *refs: partials(float(full_width), *refs),
        in_specs=[vmem] * len(stats) + [scalars, vmem],
        out_specs=[vmem] * 2,
        out_shape=[
            pltpu.VMEM((tokens // group, 3 * PAD, group * count), F32),
            pltpu.VMEM((QUARTERS * COLUMNS, width // QUARTERS), F32),
        ],
        compiler_params=params,
        name="partials",
    )(*stats, tanh_scale, in_vmem(hr))

    grads = [jax.ShapeDtypeStruct((tokens, count, width), BF16), jax.ShapeDtypeStruct((tokens, width), BF16)]

    def mixed(first, groups, last, bufs, results):
        own = groups * group
        kept = [pltpu.VMEM((own, count, width), BF16), pltpu.VMEM((own, width), BF16)]
        sems = [pltpu.SemaphoreType.DMA((2,))] * 2
        shape = (grads if bufs or last else []) + ([] if last else kept)
        done = pl.pallas_call(
            lambda *refs: outputs(first, groups, bool(bufs), last, *refs),
            in_specs=[vmem, scalars] + [vmem] * (4 + len(bufs)) + [hbm] * len(results),
            out_specs=([hbm] * 2 if bufs or last else []) + ([] if last else [vmem] * 2),
            out_shape=shape,
            scratch_shapes=(kept if last else []) + sems,
            input_output_aliases={8 + i: i for i in range(len(results))},
            compiler_params=params,
            cost_estimate=pl.CostEstimate(flops=4_000_000_000, bytes_accessed=own * width * 30, transcendentals=0),
            name="outputs",
        )(in_vmem(coef), static_mix, *map(in_vmem, (hr, gr, g0, w, *bufs)), *results)
        return ((), done) if last else (done[-2:], done[:-2])

    sizes = [tokens // group]
    if sizes[0] % WINDOWS == 0 and sizes[0] > WINDOWS:
        each = sizes[0] // WINDOWS
        sizes = [each + 1] + [each] * (WINDOWS - 2) + [each - 1]
    bufs, results, first = (), (), 0
    for index, groups in enumerate(sizes):
        bufs, results = mixed(first, groups, index == len(sizes) - 1, bufs, results)
        first += groups
    stream_grad, out_grad = results

    if dp > 1 and dp & (dp - 1) == 0:
        orders = step_orders(dp)
        for index in range(len(orders[0])):
            pairs = [
                (i * tensor + t, (i ^ orders[t % 2][index]) * tensor + t) for i in range(dp) for t in range(tensor)
            ]
            more = lax.ppermute(dw, ("dp", "tensor"), pairs)
            if index < len(orders[0]) - 1:
                dw = dw + more
    else:
        dw, more = lax.psum(dw, "dp"), jnp.zeros_like(dw)
    all_tokens = tokens * dp
    proj_scale = (float(count) * all_tokens * full_width) ** -0.5
    gain_scale = (float(count) * all_tokens) ** -0.5
    proj_grad, gain_grad = pl.pallas_call(
        lambda *refs: tail(proj_scale, gain_scale, *refs),
        in_specs=[vmem] * 4,
        out_specs=[vmem] * 2,
        out_shape=[jax.ShapeDtypeStruct((COLUMNS, width), F32), jax.ShapeDtypeStruct((1, width), F32)],
        compiler_params=params,
        name="tail",
    )(dw, more, gain.reshape(1, width), projection)
    return (stream_grad, out_grad, proj_grad, gain_grad.reshape(width))


def solution(mesh):
    placed = (
        P("dp", None, "tensor"),
        P("dp", "tensor"),
        P("dp", None, "tensor"),
        P("dp", "tensor"),
        P("tensor"),
        P(None, "tensor"),
        P(),
        P(),
    )
    return jax.shard_map(
        shards,
        mesh=mesh,
        in_specs=placed,
        out_specs=(P("dp", None, "tensor"), P("dp", "tensor"), P(None, "tensor"), P("tensor")),
        check_vma=False,
    )
```

```python
import jax
import jax.numpy as jnp
from jax import lax
from jax.experimental import pallas as pl
from jax.experimental.pallas import tpu as pltpu
from jax.sharding import PartitionSpec as P

F32 = jnp.float32
BF16 = jnp.bfloat16
HIGHEST = lax.Precision.HIGHEST
COLUMNS = 6
PAD = 8
QUARTERS = 4
STAT_TOKENS = 32
MIX_TOKENS = 16
WINDOWS = 4
DEPTHS = 4
VMEM_LIMIT = 30 * 1024 * 1024


def dot(a, b, dims, precision=None):
    return lax.dot_general(a, b, ((dims[0:1], dims[1:2]), ((), ())), precision=precision, preferred_element_type=F32)


def iota(shape, axis):
    return lax.broadcasted_iota(jnp.int32, shape, axis)


def split(value):
    high = value.astype(BF16)
    return high, (value - high.astype(F32)).astype(BF16)


def select_rows(shape, rows):
    row, lane = iota(shape, 0), iota(shape, 1)
    picked = jnp.zeros(shape, jnp.bool_)
    for index, first, count, step in rows:
        inside = (row == index) & (lane >= first) & (lane < first + count)
        picked = picked | (inside & ((lane - first) % step == 0))
    return picked.astype(F32)


def column_of(row, count):
    wanted = jnp.minimum(iota((PAD, count), 0), count - 1)
    return jnp.sum(jnp.where(iota((PAD, count), 1) == wanted, row, 0.0), axis=1, keepdims=True)


def statistics(
    h_hbm,
    g_hbm,
    y_hbm,
    g0_hbm,
    gain_hbm,
    proj_hbm,
    mix_hbm,
    scale_hbm,
    stat_ref,
    hr_ref,
    gr_ref,
    g0_ref,
    w_ref,
    table_ref,
    h_buf,
    g_buf,
    y_buf,
    gain_buf,
    proj_buf,
    mix_buf,
    scale_buf,
    sems,
    more_sems,
):
    total, streams, width = h_hbm.shape
    blocks = sems.shape[0]
    tokens = total // blocks
    weights = [
        pltpu.make_async_copy(gain_hbm, gain_buf, more_sems.at[0]),
        pltpu.make_async_copy(proj_hbm, proj_buf, more_sems.at[1]),
        pltpu.make_async_copy(mix_hbm, mix_buf, more_sems.at[2]),
        pltpu.make_async_copy(scale_hbm, scale_buf, more_sems.at[3]),
    ]

    def copies(block):
        at = pl.ds(pl.multiple_of(block * tokens, tokens), tokens)
        pairs = [(h_hbm, h_buf), (g_hbm, g_buf), (g0_hbm, g0_ref), (y_hbm, y_buf)]
        return [
            pltpu.make_async_copy(source.at[at], target.at[at], sems.at[block, index])
            for index, (source, target) in enumerate(pairs)
        ]

    for copy in weights:
        copy.start()
    for block in range(blocks):
        for copy in copies(block):
            copy.start(priority=min(block, 1))
    for copy in weights:
        copy.wait()
    high, low = split(gain_buf[...] * proj_buf[...])
    none = jnp.zeros((PAD - COLUMNS, width), F32)
    w_ref[...] = jnp.concatenate([high.astype(F32), none, low.astype(F32), none], axis=0).astype(BF16)

    lanes = table_ref.shape[1]
    stream = iota((PAD, lanes), 1) % streams
    static = jnp.zeros((PAD, lanes), F32)
    for j in range(streams):
        static = jnp.where(stream == j, column_of(mix_buf[j : j + 1, :], COLUMNS), static)
    table_ref[:PAD] = static
    table_ref[PAD:] = jnp.broadcast_to(column_of(scale_buf[...], scale_buf.shape[1]), (PAD, lanes))

    @pl.loop(0, blocks)
    def _(block):
        for copy in copies(block):
            copy.wait()

        statistics_of(block, tokens, stat_ref, hr_ref, gr_ref, g0_ref, w_ref, h_buf, g_buf, y_buf)


def statistics_of(block, tokens, stat_ref, hr_ref, gr_ref, g0_ref, w_ref, h_buf, g_buf, y_buf):
    _, streams, width = h_buf.shape
    rows = tokens * streams
    at = pl.ds(pl.multiple_of(block * tokens, tokens), tokens)
    own = pl.ds(pl.multiple_of(block * rows, rows), rows)
    product = 0.0
    depth = width // DEPTHS
    for start in range(0, width, depth):
        part = pl.ds(start, depth)
        hr_ref[own, part] = h_buf[at, :, part].reshape(rows, depth)
        gr_ref[own, part] = g_buf[at, :, part].reshape(rows, depth)
        left = jnp.concatenate([gr_ref[own, part], g0_ref[at, part], w_ref[:, part]], axis=0)
        product = product + dot(left, jnp.concatenate([hr_ref[own, part], y_buf[at, part]], axis=0), (1, 1))
    lanes = 128
    square = jnp.zeros((rows, lanes), F32)
    for start in range(0, width, lanes):
        part = hr_ref[own, pl.ds(start, lanes)].astype(F32)
        square = square + part * part
    square = jnp.sum(square.T, axis=0, keepdims=True)
    line, token = iota((rows, rows), 0), iota((rows, rows), 1) // streams
    mixer = jnp.where(line // streams == token, product[:rows, :rows], 0.0)
    mixer = jnp.sum(mixer.reshape(rows // PAD, PAD, rows), axis=0)
    folded = mixer[:streams]
    for start in range(streams, PAD, streams):
        folded = folded + mixer[start : start + streams]
    alpha = jnp.where(line[:tokens] == token[:tokens], product[rows : rows + tokens, :rows], 0.0)
    alpha = jnp.sum(alpha, axis=0, keepdims=True)
    beta = jnp.where(line[:tokens] == token[:tokens], product[:rows, rows:].T, 0.0)
    beta = jnp.sum(beta, axis=0, keepdims=True)
    lin = product[rows + tokens : rows + tokens + PAD, :rows] + product[rows + tokens + PAD :, :rows]
    stat_ref[:, own] = jnp.concatenate([beta, alpha, folded, square, jnp.zeros_like(square), lin], axis=0)


def partials(full_width, *refs):
    *stat_refs, table_ref, hr_ref, coef_ref, dw_ref = refs
    total = stat_refs[0][...]
    for ref in stat_refs[1:]:
        total = total + ref[...]
    dcoef, lin = total[:PAD], total[PAD:]
    square = dcoef[COLUMNS : COLUMNS + 1]
    inv_rms = lax.rsqrt(square / full_width + 1e-06)
    bent = jnp.tanh(inv_rms * lin)
    scales = table_ref[PAD:, 0:1]
    dpre = jnp.where(iota(bent.shape, 0) < COLUMNS, dcoef * scales * (1.0 - bent * bent), 0.0)
    dlin = dpre * inv_rms
    dsquare = -0.5 * inv_rms * inv_rms * inv_rms / full_width * jnp.sum(dpre * lin, axis=0, keepdims=True)
    high, low = split(dlin)
    left = jnp.concatenate([high.astype(F32), low.astype(F32)], axis=0).astype(BF16)
    coef = jnp.concatenate([scales * bent, dlin, jnp.broadcast_to(2.0 * dsquare, bent.shape)], axis=0)
    groups, _, lanes = coef_ref.shape
    for index in range(groups):
        coef_ref[index] = coef[:, index * lanes : (index + 1) * lanes]
    both = dot(left, hr_ref[...], (1, 0))
    dw = both[:PAD] + both[PAD:]
    part = dw.shape[1] // QUARTERS
    for q in range(QUARTERS):
        dw_ref[q * COLUMNS : (q + 1) * COLUMNS, :] = dw[:COLUMNS, q * part : (q + 1) * part]


def put(refs, first, sems):
    grad_buf, out_buf, grad_hbm, out_hbm = refs
    at = pl.ds(first, out_buf.shape[0])
    return [
        pltpu.make_async_copy(grad_buf, grad_hbm.at[at], sems.at[0]),
        pltpu.make_async_copy(out_buf, out_hbm.at[at], sems.at[1]),
    ]


def outputs(first, groups, finished, last, coef_ref, table_ref, hr_ref, gr_ref, g0_ref, w_ref, *refs):
    *results, grad_buf, out_buf, sems, more_sems = refs
    group, streams, width = grad_buf.shape[0] // groups, grad_buf.shape[1], grad_buf.shape[2]
    copies = put((*refs[:2], *results[-2:]), first * group - refs[1].shape[0], sems) if finished else []
    for copy in copies:
        copy.start()
    rows = group * streams
    at_g0, at_w, at_h, end = rows, rows + group, rows + group + 2 * PAD, 2 * rows + group + 2 * PAD
    spread = [(1, at_g0, group, 1), (2 * PAD, at_h, rows, 1)]
    spread += [(2 + k, k, rows - k, streams) for k in range(streams)]
    spread += [(PAD + c, at_w + c, PAD + 1, PAD) for c in range(COLUMNS)]
    spread = select_rows((3 * PAD, end), spread)
    token, line, lane = iota((rows, end), 0) // streams, iota((rows, end), 0), iota((rows, end), 1)
    kept = ((lane < at_g0) & (lane // streams == token)) | (lane - at_g0 == token) | (lane - at_h == line)
    kept = kept | ((lane >= at_w) & (lane < at_h))
    out_token, out_lane = iota((group, end), 0), iota((group, end), 1)
    out_kept = (out_lane < at_g0) & (out_lane // streams == out_token)
    static = table_ref[:PAD, :rows]
    lefts = []
    for index in range(groups):
        here = coef_ref[first + index]
        here = jnp.concatenate([static + here[:PAD], here[PAD:]], axis=0)
        high, low = split(jnp.where(kept, dot(here, spread, (0, 0), HIGHEST), 0.0))
        beta = jnp.concatenate([here[0:1], jnp.zeros((1, end - rows), F32)], axis=1)
        out_high, out_low = split(jnp.where(out_kept, jnp.broadcast_to(beta, (group, end)), 0.0))
        lefts.append(jnp.concatenate([high, low, out_high, out_low], axis=0))
    step = min(width, 1024)
    for index, left in enumerate(lefts):
        own = pl.ds((first + index) * rows, rows)
        source = pl.ds((first + index) * group, group)
        target = pl.ds(index * group, group)
        for column in range(0, width, step):
            at = pl.ds(column, step)
            right = jnp.concatenate([gr_ref[own, at], g0_ref[source, at], w_ref[:, at], hr_ref[own, at]], axis=0)
            result = dot(left, right, (1, 0))
            total = result[:rows] + result[rows : 2 * rows]
            grad_buf[target, :, at] = total.astype(BF16).reshape(group, streams, step)
            out_buf[target, at] = (result[2 * rows : 2 * rows + group] + result[2 * rows + group :]).astype(BF16)
    if last:
        own = put((grad_buf, out_buf, *results[-2:]), first * group, more_sems)
        for copy in own:
            copy.start()
        copies += own
    for copy in copies:
        copy.wait()


def tail(proj_scale, gain_scale, dw_ref, more_ref, gain_ref, proj_ref, proj_grad_ref, gain_grad_ref):
    dw = dw_ref[...] + more_ref[...]
    part = dw.shape[1]
    for q in range(QUARTERS):
        at = pl.ds(q * part, part)
        own = dw[q * COLUMNS : (q + 1) * COLUMNS]
        proj_grad_ref[:, at] = gain_ref[:, at] * own * proj_scale
        gain_grad_ref[:, at] = jnp.sum(own * proj_ref[:, at], axis=0, keepdims=True) * gain_scale


def step_orders(devices):
    steps = [1 << bit for bit in range(devices.bit_length() - 1)]
    half = len(steps) // 2
    even, odd = [], []
    for near, far in zip(steps[:half], steps[half:]):
        even += [near, far]
        odd += [far, near]
    return even + steps[2 * half :], odd + steps[2 * half :]


def shards(streams, layer_out, cotangent, input_cot, gain, projection, static_mix, tanh_scale):
    tokens, count, width = streams.shape
    rows = tokens * count
    dp, tensor = lax.axis_size("dp"), lax.axis_size("tensor")
    full_width = width * tensor
    params = pltpu.CompilerParams(vmem_limit_bytes=VMEM_LIMIT)

    block = min(STAT_TOKENS, tokens)
    def in_hbm(array):
        return pltpu.with_memory_space_constraint(array, pltpu.HBM)

    def in_vmem(array):
        return pltpu.with_memory_space_constraint(array, pltpu.VMEM)

    streams, cotangent, layer_out, input_cot = map(in_hbm, (streams, cotangent, layer_out, input_cot))
    vmem = pl.BlockSpec(memory_space=pltpu.VMEM)
    hbm = pl.BlockSpec(memory_space=pltpu.HBM)
    stat, hr, gr, g0, w, table = pl.pallas_call(
        statistics,
        in_specs=[hbm] * 8,
        out_specs=[vmem] * 6,
        out_shape=[
            pltpu.VMEM((2 * PAD, rows), F32),
            pltpu.VMEM((rows, width), BF16),
            pltpu.VMEM((rows, width), BF16),
            pltpu.VMEM((tokens, width), BF16),
            pltpu.VMEM((2 * PAD, width), BF16),
            pltpu.VMEM((2 * PAD, 128), F32),
        ],
        scratch_shapes=[
            pltpu.VMEM(streams.shape, BF16),
            pltpu.VMEM(streams.shape, BF16),
            pltpu.VMEM(layer_out.shape, BF16),
            pltpu.VMEM((1, width), F32),
            pltpu.VMEM((COLUMNS, width), F32),
            pltpu.VMEM(static_mix.shape, F32),
            pltpu.VMEM((1, *tanh_scale.shape), F32),
            pltpu.SemaphoreType.DMA((tokens // block, 4)),
            pltpu.SemaphoreType.DMA((4,)),
        ],
        compiler_params=params,
        name="statistics",
    )(
        *(streams, cotangent, layer_out, input_cot),
        *map(in_hbm, (gain.reshape(1, width), projection, static_mix, tanh_scale.reshape(1, -1))),
    )

    if tensor == 2:
        stats = (stat, lax.ppermute(stat, "tensor", [(0, 1), (1, 0)]))
    else:
        stats = (lax.psum(stat, "tensor"),)

    group = min(MIX_TOKENS, tokens)
    coef, dw = pl.pallas_call(
        lambda *refs: partials(float(full_width), *refs),
        in_specs=[vmem] * (len(stats) + 2),
        out_specs=[vmem] * 2,
        out_shape=[
            pltpu.VMEM((tokens // group, 3 * PAD, group * count), F32),
            pltpu.VMEM((QUARTERS * COLUMNS, width // QUARTERS), F32),
        ],
        compiler_params=params,
        name="partials",
    )(*stats, in_vmem(table), in_vmem(hr))

    grads = [jax.ShapeDtypeStruct((tokens, count, width), BF16), jax.ShapeDtypeStruct((tokens, width), BF16)]

    def mixed(first, groups, last, bufs, results):
        own = groups * group
        kept = [pltpu.VMEM((own, count, width), BF16), pltpu.VMEM((own, width), BF16)]
        sems = [pltpu.SemaphoreType.DMA((2,))] * 2
        shape = (grads if bufs or last else []) + ([] if last else kept)
        done = pl.pallas_call(
            lambda *refs: outputs(first, groups, bool(bufs), last, *refs),
            in_specs=[vmem] * (6 + len(bufs)) + [hbm] * len(results),
            out_specs=([hbm] * 2 if bufs or last else []) + ([] if last else [vmem] * 2),
            out_shape=shape,
            scratch_shapes=(kept if last else []) + sems,
            input_output_aliases={8 + i: i for i in range(len(results))},
            compiler_params=params,
            cost_estimate=pl.CostEstimate(flops=4_000_000_000, bytes_accessed=own * width * 30, transcendentals=0),
            name="outputs",
        )(*map(in_vmem, (coef, table)), *map(in_vmem, (hr, gr, g0, w, *bufs)), *results)
        return ((), done) if last else (done[-2:], done[:-2])

    sizes = [tokens // group]
    if sizes[0] % WINDOWS == 0 and sizes[0] > WINDOWS:
        each = sizes[0] // WINDOWS
        sizes = [each + 1] + [each] * (WINDOWS - 2) + [each - 1]
    bufs, results, first = (), (), 0
    for index, groups in enumerate(sizes):
        bufs, results = mixed(first, groups, index == len(sizes) - 1, bufs, results)
        first += groups
    stream_grad, out_grad = results

    if dp > 1 and dp & (dp - 1) == 0:
        orders = step_orders(dp)
        for index in range(len(orders[0])):
            pairs = [
                (i * tensor + t, (i ^ orders[t % 2][index]) * tensor + t) for i in range(dp) for t in range(tensor)
            ]
            more = lax.ppermute(dw, ("dp", "tensor"), pairs)
            if index < len(orders[0]) - 1:
                dw = dw + more
    else:
        dw, more = lax.psum(dw, "dp"), jnp.zeros_like(dw)
    all_tokens = tokens * dp
    proj_scale = (float(count) * all_tokens * full_width) ** -0.5
    gain_scale = (float(count) * all_tokens) ** -0.5
    proj_grad, gain_grad = pl.pallas_call(
        lambda *refs: tail(proj_scale, gain_scale, *refs),
        in_specs=[vmem] * 4,
        out_specs=[vmem] * 2,
        out_shape=[jax.ShapeDtypeStruct((COLUMNS, width), F32), jax.ShapeDtypeStruct((1, width), F32)],
        compiler_params=params,
        name="tail",
    )(dw, more, gain.reshape(1, width), projection)
    return (stream_grad, out_grad, proj_grad, gain_grad.reshape(width))


def solution(mesh):
    placed = (
        P("dp", None, "tensor"),
        P("dp", "tensor"),
        P("dp", None, "tensor"),
        P("dp", "tensor"),
        P("tensor"),
        P(None, "tensor"),
        P(),
        P(),
    )
    return jax.shard_map(
        shards,
        mesh=mesh,
        in_specs=placed,
        out_specs=(P("dp", None, "tensor"), P("dp", "tensor"), P(None, "tensor"), P("tensor")),
        check_vma=False,
    )
```
